512 devices in a mesh: rows: 128 (over y, z, core), rank: 4 (over x).
Axes of the slice: x: 4, y: 8, z: 8, core: 2. Of those that a mesh axis runs over, the one named last changes fastest.
Arguments:
- left_factor: bfloat16 [128, 262144], P(None, 'rows'), may hold values from -8 to 8
- right_factor: bfloat16 [128, 262144], P(None, 'rows'), may hold values from -8 to 8
- left_plan: float32 [256, 262144], P('rank', 'rows'), may hold values from 0.0068 to 147, as said below
- right_plan: float32 [256, 262144], P('rank', 'rows'), may hold values from 0.0068 to 147, as said below
- log_inner: float32 [256], P('rank'), may hold values from -1 to 1
- left_mass: float32 [262144], P('rows'), may hold values from 32 to 1024, as said below
- right_mass: float32 [262144], P('rows'), may hold values from 32 to 1024, as said below
Outputs:
- new_left: float32 [256, 262144], P('rank', 'rows')
- new_right: float32 [256, 262144], P('rank', 'rows')
- new_log_inner: float32 [256], P('rank')
The draws below stay inside these ranges and needn't reach their ends.
Inputs may be any that keep to these rules, and one draw needn't show every extreme that they name: `left_plan`: positive entries. `right_plan`: positive entries. `left_mass`: positive point masses. `right_mass`: positive point masses.
All inputs are finite; a program needn't handle non-finite values. Where the reference program divides by a largest or mean magnitude, that divisor is 1e-20 or more.
Results may differ from the reference program's by a relative error of at most 0.00045.
Values sent between devices are 32-bit elements; how exact they have to be, the bound alone decides.
A program may use at most 64 MiB of HBM per device.

```python
import math
import jax
import jax.numpy as jnp
from jax import lax

DC = 128
RANK = 256
ROWS_DEV = 2048
ITERS = 3
POINTS = 262144


def draw_masses(key):
    blocks = POINTS // ROWS_DEV
    level = jnp.exp(jax.random.uniform(jax.random.fold_in(key, 1), (blocks, 1), jnp.float32, math.log(32.0), math.log(512.0)))
    factor = jax.random.uniform(jax.random.fold_in(key, 2), (blocks, ROWS_DEV), jnp.float32, 1.0, 2.0)
    return (level * factor).reshape(POINTS)


def draw_left_mass(key, part):
    return draw_masses(jax.random.fold_in(key, 11))


def draw_right_mass(key, part):
    return draw_masses(jax.random.fold_in(key, 23))


def draw_points(key, salt):
    blocks = POINTS // ROWS_DEV
    inner_key = jax.random.fold_in(key, salt)
    offset = jax.random.uniform(jax.random.fold_in(inner_key, 5), (blocks, 1), jnp.float32, -1.25, 1.25)
    offset = jnp.broadcast_to(offset, (blocks, ROWS_DEV)).reshape(1, POINTS)
    noise = jax.random.truncated_normal(jax.random.fold_in(inner_key, 2), -2.75, 2.75, (DC, POINTS), jnp.float32)
    return jnp.clip(noise + offset, -4.0, 4.0)


def draw_directions(key):
    return jax.random.normal(jax.random.fold_in(key, 307), (DC, RANK), jnp.float32) / math.sqrt(DC)


def draw_plan(key, salt):
    blocks = POINTS // ROWS_DEV
    inner_key = jax.random.fold_in(key, salt)
    points = draw_points(key, salt)
    directions = draw_directions(key)
    align = jnp.dot(directions.T, points, precision=lax.Precision.HIGHEST)
    align = jnp.clip(align, -3.0, 3.0).reshape(RANK, blocks, ROWS_DEV)
    strength = jax.random.uniform(jax.random.fold_in(inner_key, 3), (1, blocks, 1), jnp.float32, 0.4, 1.2)
    leaning = jnp.exp(strength * align).reshape(RANK, POINTS)
    base = jnp.exp(jax.random.uniform(jax.random.fold_in(inner_key, 4), (RANK, POINTS), jnp.float32, math.log(0.25), math.log(4.0)))
    return base * leaning


def draw_left_factor(key, part):
    return (2.0 * draw_points(key, 101)).astype(jnp.bfloat16)


def draw_right_factor(key, part):
    return (2.0 * draw_points(key, 202)).astype(jnp.bfloat16)


def draw_left_plan(key, part):
    return draw_plan(key, 101)


def draw_right_plan(key, part):
    return draw_plan(key, 202)


def shard_levels(key, extent, split, low, top_value):
    def one(position, parts):
        heights = jax.random.uniform(jax.random.fold_in(jax.random.fold_in(key, 6), position), (parts,), jnp.float32, low / len(split), top_value / len(split))
        return jnp.repeat(jnp.exp(heights), extent[position] // parts).reshape((-1,) + (1,) * (len(extent) - position - 1))

    loudness = one(*split[0])
    for cut in split[1:]:
        loudness = loudness * one(*cut)
    return loudness


def setup_inputs(seed: int = 0) -> dict:
    keys = jax.random.split(jax.random.key(seed), 8)
    left_factor = draw_left_factor(jax.random.fold_in(keys[7], 71), 0)
    right_factor = draw_right_factor(jax.random.fold_in(keys[7], 71), 0)
    left_plan = draw_left_plan(jax.random.fold_in(keys[7], 71), 0)
    right_plan = draw_right_plan(jax.random.fold_in(keys[7], 71), 0)
    log_inner = jnp.clip(jax.random.uniform(keys[4], (RANK,), jnp.float32, -1.0, 1.0) * shard_levels(keys[4], (RANK,), ((0, 4),), -0.4, 0.0), -1.0, 1.0)
    left_mass = draw_left_mass(jax.random.fold_in(keys[7], 71), 0)
    right_mass = draw_right_mass(jax.random.fold_in(keys[7], 71), 0)
    return {"left_factor": left_factor, "right_factor": right_factor, "left_plan": left_plan, "right_plan": right_plan, "log_inner": log_inner, "left_mass": left_mass, "right_mass": right_mass}


def balance(inner_mass, col_scale_left, col_total_left, col_scale_right, col_total_right):
    mixed = jnp.log(inner_mass) + jnp.log(col_scale_left * col_total_left) + jnp.log(col_scale_right * col_total_right)
    inner_mass = jnp.exp(mixed / 3.0)
    return inner_mass, inner_mass / col_total_left, inner_mass / col_total_right


def reference(left_factor, right_factor, left_plan, right_plan, log_inner, left_mass, right_mass):
    precise = lax.Precision.HIGHEST
    total_left = jnp.sum(left_mass)
    total_right = jnp.sum(right_mass)
    inner_mass = (total_left / RANK) * jnp.exp(log_inner)
    left_round = left_plan.astype(jnp.bfloat16)
    right_round = right_plan.astype(jnp.bfloat16)
    proj_right = jnp.dot(right_factor, right_round.T, preferred_element_type=jnp.float32)
    proj_left = jnp.dot(left_factor, left_round.T, preferred_element_type=jnp.float32)
    scaled_right = (proj_right / inner_mass[None, :]).astype(jnp.bfloat16)
    scaled_left = (proj_left / inner_mass[None, :]).astype(jnp.bfloat16)
    grad_left = jnp.dot(scaled_right.T, left_factor, preferred_element_type=jnp.float32)
    grad_right = jnp.dot(scaled_left.T, right_factor, preferred_element_type=jnp.float32)
    pairing = jnp.sum(left_round.astype(jnp.float32) * grad_left, axis=1)
    grad_inner = -pairing / inner_mass
    largest = jnp.maximum(jnp.maximum(jnp.max(jnp.abs(grad_left)), jnp.max(jnp.abs(grad_right))), jnp.max(jnp.abs(grad_inner)))
    step_size = 5.0 / jnp.maximum(largest, 0.25)
    tilted_left = left_plan * jnp.exp(-step_size * grad_left)
    tilted_right = right_plan * jnp.exp(-step_size * grad_right)
    inner_mass = inner_mass * jnp.exp(-step_size * grad_inner)
    right_norm = right_mass * (total_left / total_right)
    col_scale_left = jnp.ones((RANK,), jnp.float32)
    col_scale_right = jnp.ones((RANK,), jnp.float32)
    row_scale_left = left_mass
    row_scale_right = right_norm
    for repeat in range(ITERS):
        row_scale_left = left_mass / jnp.dot(col_scale_left, tilted_left, precision=precise)
        row_scale_right = right_norm / jnp.dot(col_scale_right, tilted_right, precision=precise)
        col_total_left = jnp.dot(tilted_left, row_scale_left, precision=precise)
        col_total_right = jnp.dot(tilted_right, row_scale_right, precision=precise)
        inner_mass, col_scale_left, col_scale_right = balance(inner_mass, col_scale_left, col_total_left, col_scale_right, col_total_right)
    new_left = row_scale_left[None, :] * tilted_left * col_scale_left[:, None]
    new_right = row_scale_right[None, :] * tilted_right * col_scale_right[:, None]
    new_log_inner = jnp.log(inner_mass) - jnp.log(total_left / RANK)
    return new_left, new_right, new_log_inner
```

```python
import functools

import jax
import jax.numpy as jnp
from jax import lax
from jax.experimental import pallas as pl
from jax.experimental.pallas import tpu as pltpu
from jax.sharding import Mesh
from jax.sharding import PartitionSpec as P

ITERS = 3
LANES = 128
ROWS = ("y", "z", "c")
F32 = jnp.float32


def far_first(size):
    return sorted(range(1, size), key=lambda d: -min(d, size - d))


def kernel(
    sizes,
    lf_hbm,
    rf_hbm,
    lp_hbm,
    rp_hbm,
    li_ref,
    lm_ref,
    rm_ref,
    ol_hbm,
    or_hbm,
    oi_ref,
    lf,
    rf,
    plan,
    grad,
    src,
    r1,
    r2,
    full,
    m1,
    m2,
    rx,
    rs,
    c1,
    c2,
    load_sem,
    store_sem,
    send_sem,
    recv_sem,
):
    ny, nz, nc, nx = sizes
    half = LANES // 2
    points = lf.shape[1]
    tiles = points // LANES
    rank = half * nx
    y, z, c, x = (lax.axis_index(a) for a in ("y", "z", "c", "x"))
    yc_size, zx_size = ny * nc, nz * nx
    yc, zx = y * nc + c, z * nx + x
    piece = LANES // yc_size

    yc_peers = [
        {"y": lax.rem(y + dy, ny), "c": lax.rem(c + dc, nc)}
        for dy in far_first(ny) + [0]
        for dc in range(nc)
        if dy or dc
    ]
    z_peers = [{"z": lax.rem(z + dz, nz)} for dz in far_first(nz)]
    x_peers = [{"x": lax.rem(x + dx, nx)} for dx in far_first(nx)]
    zx_peers = [
        {"z": lax.rem(z + dz, nz), "x": lax.rem(x + dx, nx)}
        for dz in far_first(nz) + [0]
        for dx in far_first(nx) + [0]
        if dz or dx
    ]

    loads = [
        pltpu.make_async_copy(a, b, load_sem.at[i])
        for i, (a, b) in enumerate(
            (
                (rp_hbm, plan.at[half:]),
                (rf_hbm, rf),
                (lp_hbm, plan.at[:half]),
                (lf_hbm, lf),
            )
        )
    ]
    for load in loads:
        load.start()
    barrier = pltpu.get_barrier_semaphore()
    greeted = zx_peers + yc_peers
    for peer in greeted:
        pl.semaphore_signal(
            barrier, inc=1, device_id=peer, device_id_type=pl.DeviceIdType.MESH
        )

    def send(stage, source, target, peer):
        pltpu.make_async_remote_copy(
            src_ref=source,
            dst_ref=target,
            send_sem=send_sem.at[stage],
            recv_sem=recv_sem.at[stage],
            device_id=peer,
            device_id_type=pl.DeviceIdType.MESH,
        ).start()

    sent = []

    def spread(stage, ref, peers):
        for peer in peers:
            send(stage, ref, ref, peer)

    def arrived(stage, bulk):
        pltpu.make_async_copy(bulk, bulk, recv_sem.at[stage]).wait()
        sent.append((stage, bulk))

    lane = lax.broadcasted_iota(jnp.int32, (1, LANES), 1)
    low = lane < half
    eye = lax.broadcasted_iota(jnp.int32, (LANES, LANES), 0) == lax.broadcasted_iota(
        jnp.int32, (LANES, LANES), 1
    )

    def to_column(row):
        return jnp.sum(jnp.where(eye, row, 0.0), axis=1, keepdims=True)

    def to_row(column):
        return jnp.sum(jnp.where(eye, column, 0.0), axis=0, keepdims=True)

    def swap(row):
        return jnp.concatenate([row[:, half:], row[:, :half]], axis=1)

    def product(rows, factor):
        return lax.dot_general(
            plan[rows, :].astype(jnp.bfloat16),
            factor[...],
            (((1,), (1,)), ((), ())),
            preferred_element_type=F32,
        )

    lower, upper = slice(0, half), slice(half, LANES)
    mass_left = jnp.sum(lm_ref[...], axis=0, keepdims=True)
    mass_right = jnp.sum(rm_ref[...], axis=0, keepdims=True)
    masses = jnp.where(low, mass_left + swap(mass_left), mass_right + swap(mass_right))
    loads[0].wait()
    loads[1].wait()
    per = half // piece
    src[0:per, 0:piece, :] = product(upper, rf).reshape(per, piece, LANES)
    loads[2].wait()
    loads[3].wait()
    src[per : 2 * per, 0:piece, :] = product(lower, lf).reshape(per, piece, LANES)
    src[:, piece : piece + 1, :] = jnp.broadcast_to(
        masses.reshape(1, 1, LANES), (yc_size, 1, LANES)
    )
    pl.semaphore_wait(barrier, len(greeted))

    for peer in yc_peers:
        send(0, src.at[peer["y"] * nc + peer["c"]], r1.at[yc], peer)
    r1[yc] = src[yc]
    log_inner = jnp.concatenate([li_ref[...], li_ref[...]], axis=1)
    inner_base = jnp.exp(to_column(log_inner))
    arrived(0, r1.at[pl.ds(0, yc_size - 1)])
    r2[z] = jnp.sum(r1[...], axis=0)
    spread(1, r2.at[z], z_peers)
    arrived(1, r2.at[pl.ds(0, nz - 1)])
    summed = jnp.sum(r2[...], axis=0)
    mine = full.at[pl.ds(pl.multiple_of(yc * piece, piece), piece)]
    mine[...] = summed[:piece]
    spread(2, mine, yc_peers)
    masses = summed[piece:]
    total_left = jnp.sum(jnp.where(low, masses, 0.0), axis=1, keepdims=True)
    total_right = jnp.sum(jnp.where(low, 0.0, masses), axis=1, keepdims=True)
    mean_left = total_left / rank
    inner = mean_left * inner_base
    log_inner = jnp.log(mean_left) + log_inner
    right_norm = rm_ref[...] * (total_left / total_right)
    arrived(2, full.at[pl.ds(0, (yc_size - 1) * piece)])

    scaled = (full[...] / inner).astype(jnp.bfloat16)
    pairing = jnp.sum(
        scaled[lower].astype(F32) * full[upper, :], axis=1, keepdims=True
    )
    grad_inner = -pairing / inner[lower]
    grad_inner = to_row(jnp.concatenate([grad_inner, grad_inner], axis=0))

    width = 512 if points % 512 == 0 else LANES
    top = jnp.zeros((half, LANES), F32)
    for rows, factor in ((lower, lf), (upper, rf)):
        for at in range(0, points, width):
            part = jnp.dot(
                scaled[rows], factor[:, at : at + width], preferred_element_type=F32
            )
            grad[rows, at : at + width] = part
            part = jnp.abs(part)
            for k in range(0, width, LANES):
                top = jnp.maximum(top, part[:, k : k + LANES])
    top = jnp.maximum(jnp.max(top, axis=0, keepdims=True), jnp.abs(grad_inner))

    m1[yc] = top
    spread(3, m1.at[yc], yc_peers)
    arrived(3, m1.at[pl.ds(0, yc_size - 1)])
    m2[zx] = jnp.max(m1[...], axis=0)
    spread(4, m2.at[zx], zx_peers)
    arrived(4, m2.at[pl.ds(0, zx_size - 1)])
    largest = jnp.max(jnp.max(m2[...], axis=0), axis=1, keepdims=True)
    step = 5.0 / jnp.maximum(largest, 0.25)

    sides = ((0, lower, lm_ref[...]), (1, upper, right_norm))
    log_inner = log_inner - step * grad_inner
    scale_row = jnp.ones((1, LANES), F32)
    scale = None
    stage = 5
    for turn in range(ITERS):
        for side, rows, _ in sides:
            for t in range(tiles):
                at = slice(t * LANES, (t + 1) * LANES)
                if turn == 0:
                    tilted = plan[rows, at] * jnp.exp(-step * grad[rows, at])
                    plan[rows, at] = tilted
                else:
                    tilted = plan[rows, at] * scale[rows]
                rx[turn, side, x, t : t + 1, :] = jnp.sum(tilted, axis=0, keepdims=True)
            spread(stage + side, rx.at[turn, side, x], x_peers)
        sums = []
        for side, rows, mass in sides:
            arrived(stage + side, rx.at[turn, side, pl.ds(0, nx - 1)])
            rs[side] = mass / jnp.sum(rx[turn, side], axis=0)
            acc = jnp.zeros((half, LANES), F32)
            for t in range(tiles):
                acc += plan[rows, t * LANES : (t + 1) * LANES] * rs[side, t : t + 1, :]
            sums.append(jnp.sum(acc, axis=1, keepdims=True))
        c1[turn, yc] = to_row(jnp.concatenate(sums, axis=0))
        spread(stage + 2, c1.at[turn, yc], yc_peers)
        arrived(stage + 2, c1.at[turn, pl.ds(0, yc_size - 1)])
        c2[turn, z] = jnp.sum(c1[turn], axis=0)
        spread(stage + 3, c2.at[turn, z], z_peers)
        arrived(stage + 3, c2.at[turn, pl.ds(0, nz - 1)])
        totals = jnp.sum(c2[turn], axis=0)
        mixed = jnp.log(scale_row * totals)
        log_inner = (log_inner + (mixed + swap(mixed))) / 3.0
        scale_row = jnp.exp(log_inner) / totals
        scale = to_column(scale_row)
        stage += 4

    oi_ref[...] = (log_inner - jnp.log(mean_left))[:, :half]
    stores = []
    for side, rows, _ in sides:
        for t in range(tiles):
            at = slice(t * LANES, (t + 1) * LANES)
            grad[rows, at] = rs[side, t : t + 1, :] * plan[rows, at] * scale[rows]
        store = pltpu.make_async_copy(
            grad.at[rows], (ol_hbm, or_hbm)[side], store_sem.at[side]
        )
        store.start()
        stores.append(store)
    for number, bulk in sent:
        pltpu.make_async_copy(bulk, bulk, send_sem.at[number]).wait()
    for store in stores:
        store.wait()


def per_device(
    sizes, left_factor, right_factor, left_plan, right_plan, log_inner, left_mass, right_mass
):
    ny, nz, nc, nx = sizes
    depth, points = left_factor.shape
    columns = left_plan.shape[0]
    tiles = points // LANES
    yc_size, zx_size = ny * nc, nz * nx
    piece = LANES // yc_size
    stages = 5 + 4 * ITERS
    hbm = pl.BlockSpec(memory_space=pl.ANY)
    vmem = pl.BlockSpec(memory_space=pltpu.VMEM)
    new_left, new_right, new_log_inner = pl.pallas_call(
        functools.partial(kernel, sizes),
        out_shape=(
            jax.ShapeDtypeStruct((columns, points), F32),
            jax.ShapeDtypeStruct((columns, points), F32),
            jax.ShapeDtypeStruct((1, columns), F32),
        ),
        in_specs=[hbm] * 4 + [vmem] * 3,
        out_specs=(hbm, hbm, vmem),
        scratch_shapes=[
            pltpu.VMEM((depth, points), jnp.bfloat16),
            pltpu.VMEM((depth, points), jnp.bfloat16),
            pltpu.VMEM((2 * columns, points), F32),
            pltpu.VMEM((2 * columns, points), F32),
            pltpu.VMEM((yc_size, piece + 1, LANES), F32),
            pltpu.VMEM((yc_size, piece + 1, LANES), F32),
            pltpu.VMEM((nz, piece + 1, LANES), F32),
            pltpu.VMEM((LANES, LANES), F32),
            pltpu.VMEM((yc_size, 1, LANES), F32),
            pltpu.VMEM((zx_size, 1, LANES), F32),
            pltpu.VMEM((ITERS, 2, nx, tiles, LANES), F32),
            pltpu.VMEM((2, tiles, LANES), F32),
            pltpu.VMEM((ITERS, yc_size, 1, LANES), F32),
            pltpu.VMEM((ITERS, nz, 1, LANES), F32),
            pltpu.SemaphoreType.DMA((4,)),
            pltpu.SemaphoreType.DMA((2,)),
            pltpu.SemaphoreType.DMA((stages,)),
            pltpu.SemaphoreType.DMA((stages,)),
        ],
        compiler_params=pltpu.CompilerParams(collective_id=0, has_side_effects=True),
    )(
        left_factor,
        right_factor,
        left_plan,
        right_plan,
        log_inner.reshape(1, columns),
        left_mass.reshape(tiles, LANES),
        right_mass.reshape(tiles, LANES),
    )
    return new_left, new_right, new_log_inner.reshape(columns)


def solution(mesh):
    nx = mesh.shape["rank"]
    nc = 2
    ny = 1
    while mesh.shape["rows"] // nc > ny * ny:
        ny *= 2
    nz = mesh.shape["rows"] // (nc * ny)
    split = Mesh(mesh.devices.reshape(ny, nz, nc, nx), ("y", "z", "c", "x"))
    placed = (
        P(None, ROWS),
        P(None, ROWS),
        P("x", ROWS),
        P("x", ROWS),
        P("x"),
        P(ROWS),
        P(ROWS),
    )
    return jax.shard_map(
        functools.partial(per_device, (ny, nz, nc, nx)),
        mesh=split,
        in_specs=placed,
        out_specs=(P("x", ROWS), P("x", ROWS), P("x")),
        check_vma=False,
    )
```

```python
import functools

import jax
import jax.numpy as jnp
from jax import lax
from jax.experimental import pallas as pl
from jax.experimental.pallas import tpu as pltpu
from jax.sharding import Mesh
from jax.sharding import PartitionSpec as P

ITERS = 3
LANES = 128
ROWS = ("y", "z", "c")
F32 = jnp.float32


def far_first(size):
    return sorted(range(1, size), key=lambda d: -min(d, size - d))


def kernel(
    sizes,
    lf_hbm,
    rf_hbm,
    lp_hbm,
    rp_hbm,
    li_ref,
    lm_ref,
    rm_ref,
    plan,
    rs,
    scale_ref,
    oi_ref,
    lf,
    rf,
    grad,
    src,
    r1,
    r2,
    full,
    m1,
    m2,
    rx,
    c1,
    load_sem,
    send_sem,
    recv_sem,
):
    ny, nz, nc, nx = sizes
    half = LANES // 2
    points = lf.shape[1]
    tiles = points // LANES
    rank = half * nx
    y, z, c, x = (lax.axis_index(a) for a in ("y", "z", "c", "x"))
    yc_size, zx_size, row_size = ny * nc, nz * nx, ny * nz * nc
    yc, zx, row = y * nc + c, z * nx + x, (y * nz + z) * nc + c
    piece = LANES // yc_size

    row_peers = [
        {"y": lax.rem(y + dy, ny), "z": lax.rem(z + dz, nz), "c": lax.rem(c + dc, nc)}
        for dy in far_first(ny) + [0]
        for dz in far_first(nz) + [0]
        for dc in range(nc)
        if dy or dz or dc
    ]
    yc_peers = [
        {"y": lax.rem(y + dy, ny), "c": lax.rem(c + dc, nc)}
        for dy in far_first(ny) + [0]
        for dc in range(nc)
        if dy or dc
    ]
    z_peers = [{"z": lax.rem(z + dz, nz)} for dz in far_first(nz)]
    x_peers = [{"x": lax.rem(x + dx, nx)} for dx in far_first(nx)]
    zx_peers = [
        {"z": lax.rem(z + dz, nz), "x": lax.rem(x + dx, nx)}
        for dz in far_first(nz) + [0]
        for dx in far_first(nx) + [0]
        if dz or dx
    ]

    loads = [
        pltpu.make_async_copy(a, b, load_sem.at[i])
        for i, (a, b) in enumerate(
            (
                (rp_hbm, plan.at[half:]),
                (rf_hbm, rf),
                (lp_hbm, plan.at[:half]),
                (lf_hbm, lf),
            )
        )
    ]
    for load in loads:
        load.start()
    barrier = pltpu.get_barrier_semaphore()
    greeted = yc_peers + z_peers + x_peers
    for peer in greeted:
        pl.semaphore_signal(
            barrier, inc=1, device_id=peer, device_id_type=pl.DeviceIdType.MESH
        )

    def send(stage, source, target, peer):
        pltpu.make_async_remote_copy(
            src_ref=source,
            dst_ref=target,
            send_sem=send_sem.at[stage],
            recv_sem=recv_sem.at[stage],
            device_id=peer,
            device_id_type=pl.DeviceIdType.MESH,
        ).start()

    sent = []

    def spread(stage, ref, peers):
        for peer in peers:
            send(stage, ref, ref, peer)

    def arrived(stage, bulk):
        pltpu.make_async_copy(bulk, bulk, recv_sem.at[stage]).wait()
        sent.append((stage, bulk))

    lane = lax.broadcasted_iota(jnp.int32, (1, LANES), 1)
    low = lane < half
    eye = lax.broadcasted_iota(jnp.int32, (LANES, LANES), 0) == lax.broadcasted_iota(
        jnp.int32, (LANES, LANES), 1
    )

    def to_column(row):
        return jnp.sum(jnp.where(eye, row, 0.0), axis=1, keepdims=True)

    def to_row(column):
        return jnp.sum(jnp.where(eye, column, 0.0), axis=0, keepdims=True)

    def swap(row):
        return jnp.concatenate([row[:, half:], row[:, :half]], axis=1)

    def product(rows, factor):
        return lax.dot_general(
            plan[rows, :].astype(jnp.bfloat16),
            factor[...],
            (((1,), (1,)), ((), ())),
            preferred_element_type=F32,
        )

    lower, upper = slice(0, half), slice(half, LANES)
    mass_left = jnp.sum(lm_ref[...], axis=0, keepdims=True)
    mass_right = jnp.sum(rm_ref[...], axis=0, keepdims=True)
    masses = jnp.where(low, mass_left + swap(mass_left), mass_right + swap(mass_right))
    loads[0].wait()
    loads[1].wait()
    per = half // piece
    src[0:per, 0:piece, :] = product(upper, rf).reshape(per, piece, LANES)
    loads[2].wait()
    loads[3].wait()
    src[per : 2 * per, 0:piece, :] = product(lower, lf).reshape(per, piece, LANES)
    src[:, piece : piece + 1, :] = jnp.broadcast_to(
        masses.reshape(1, 1, LANES), (yc_size, 1, LANES)
    )
    pl.semaphore_wait(barrier, len(greeted))

    for peer in yc_peers:
        send(0, src.at[peer["y"] * nc + peer["c"]], r1.at[yc], peer)
    r1[yc] = src[yc]
    log_inner = jnp.concatenate([li_ref[...], li_ref[...]], axis=1)
    inner_base = jnp.exp(to_column(log_inner))
    arrived(0, r1.at[pl.ds(0, yc_size - 1)])
    r2[z] = jnp.sum(r1[...], axis=0)
    spread(1, r2.at[z], z_peers)
    arrived(1, r2.at[pl.ds(0, nz - 1)])
    summed = jnp.sum(r2[...], axis=0)
    mine = full.at[pl.ds(pl.multiple_of(yc * piece, piece), piece)]
    mine[...] = summed[:piece]
    spread(2, mine, yc_peers)
    masses = summed[piece:]
    total_left = jnp.sum(jnp.where(low, masses, 0.0), axis=1, keepdims=True)
    total_right = jnp.sum(jnp.where(low, 0.0, masses), axis=1, keepdims=True)
    mean_left = total_left / rank
    inner = mean_left * inner_base
    log_inner = jnp.log(mean_left) + log_inner
    right_norm = rm_ref[...] * (total_left / total_right)
    arrived(2, full.at[pl.ds(0, (yc_size - 1) * piece)])

    scaled = (full[...] / inner).astype(jnp.bfloat16)
    pairing = jnp.sum(
        scaled[lower].astype(F32) * full[upper, :], axis=1, keepdims=True
    )
    grad_inner = -pairing / inner[lower]
    grad_inner = to_row(jnp.concatenate([grad_inner, grad_inner], axis=0))

    width = 512 if points % 512 == 0 else LANES
    top = jnp.zeros((half, LANES), F32)
    for rows, factor in ((lower, lf), (upper, rf)):
        for at in range(0, points, width):
            part = jnp.dot(
                scaled[rows], factor[:, at : at + width], preferred_element_type=F32
            )
            grad[rows, at : at + width] = part
            part = jnp.abs(part)
            for k in range(0, width, LANES):
                top = jnp.maximum(top, part[:, k : k + LANES])
    top = jnp.maximum(jnp.max(top, axis=0, keepdims=True), jnp.abs(grad_inner))

    m1[yc] = top
    spread(3, m1.at[yc], yc_peers)
    arrived(3, m1.at[pl.ds(0, yc_size - 1)])
    m2[zx] = jnp.max(m1[...], axis=0)
    spread(4, m2.at[zx], zx_peers)
    arrived(4, m2.at[pl.ds(0, zx_size - 1)])
    largest = jnp.max(jnp.max(m2[...], axis=0), axis=1, keepdims=True)
    step = 5.0 / jnp.maximum(largest, 0.25)

    sides = ((0, lower, lm_ref[...]), (1, upper, right_norm))
    log_inner = log_inner - step * grad_inner
    scale_row = jnp.ones((1, LANES), F32)
    scale = None
    stage = 5
    for turn in range(ITERS):
        for side, rows, _ in sides:
            for t in range(tiles):
                at = slice(t * LANES, (t + 1) * LANES)
                if turn == 0:
                    tilted = plan[rows, at] * jnp.exp(-step * grad[rows, at])
                    plan[rows, at] = tilted
                else:
                    tilted = plan[rows, at] * scale[rows]
                rx[turn, side, x, t : t + 1, :] = jnp.sum(tilted, axis=0, keepdims=True)
            spread(stage + side, rx.at[turn, side, x], x_peers)
        sums = []
        for side, rows, mass in sides:
            arrived(stage + side, rx.at[turn, side, pl.ds(0, nx - 1)])
            rs[side] = mass / jnp.sum(rx[turn, side], axis=0)
            acc = jnp.zeros((half, LANES), F32)
            for t in range(tiles):
                acc += plan[rows, t * LANES : (t + 1) * LANES] * rs[side, t : t + 1, :]
            sums.append(jnp.sum(acc, axis=1, keepdims=True))
        c1[turn, row] = to_row(jnp.concatenate(sums, axis=0))
        spread(stage + 2, c1.at[turn, row], row_peers)
        arrived(stage + 2, c1.at[turn, pl.ds(0, row_size - 1)])
        totals = jnp.sum(c1[turn], axis=0)
        mixed = jnp.log(scale_row * totals)
        log_inner = (log_inner + (mixed + swap(mixed))) / 3.0
        scale_row = jnp.exp(log_inner) / totals
        scale = to_column(scale_row)
        stage += 3

    oi_ref[...] = (log_inner - jnp.log(mean_left))[:, :half]
    scale_ref[...] = jnp.broadcast_to(scale, (LANES, LANES))
    for number, bulk in sent:
        pltpu.make_async_copy(bulk, bulk, send_sem.at[number]).wait()


def finish(tilted, rs, scale, oi_in, ol_hbm, or_hbm, oi_out, out, store_sem):
    half = LANES // 2
    oi_out[...] = oi_in[...]
    stores = []
    for side, target in ((0, ol_hbm), (1, or_hbm)):
        rows = slice(side * half, (side + 1) * half)
        for t in range(rs.shape[1]):
            at = slice(t * LANES, (t + 1) * LANES)
            out[rows, at] = rs[side, t : t + 1, :] * tilted[rows, at] * scale[rows, :]
        store = pltpu.make_async_copy(out.at[rows], target, store_sem.at[side])
        store.start()
        stores.append(store)
    for store in stores:
        store.wait()


def per_device(
    sizes, left_factor, right_factor, left_plan, right_plan, log_inner, left_mass, right_mass
):
    ny, nz, nc, nx = sizes
    depth, points = left_factor.shape
    columns = left_plan.shape[0]
    tiles = points // LANES
    yc_size, zx_size = ny * nc, nz * nx
    piece = LANES // yc_size
    row_size = ny * nz * nc
    stages = 5 + 3 * ITERS
    hbm = pl.BlockSpec(memory_space=pltpu.HBM)
    vmem = pl.BlockSpec(memory_space=pltpu.VMEM)
    tilted, row_scale, col_scale, new_log_inner = pl.pallas_call(
        functools.partial(kernel, sizes),
        out_shape=(
            pltpu.VMEM((2 * columns, points), F32),
            pltpu.VMEM((2, tiles, LANES), F32),
            pltpu.VMEM((LANES, LANES), F32),
            pltpu.VMEM((1, columns), F32),
        ),
        in_specs=[hbm] * 4 + [vmem] * 3,
        out_specs=(vmem, vmem, vmem, vmem),
        scratch_shapes=[
            pltpu.VMEM((depth, points), jnp.bfloat16),
            pltpu.VMEM((depth, points), jnp.bfloat16),
            pltpu.VMEM((2 * columns, points), F32),
            pltpu.VMEM((yc_size, piece + 1, LANES), F32),
            pltpu.VMEM((yc_size, piece + 1, LANES), F32),
            pltpu.VMEM((nz, piece + 1, LANES), F32),
            pltpu.VMEM((LANES, LANES), F32),
            pltpu.VMEM((yc_size, 1, LANES), F32),
            pltpu.VMEM((zx_size, 1, LANES), F32),
            pltpu.VMEM((ITERS, 2, nx, tiles, LANES), F32),
            pltpu.VMEM((ITERS, row_size, 1, LANES), F32),
            pltpu.SemaphoreType.DMA((4,)),
            pltpu.SemaphoreType.DMA((stages,)),
            pltpu.SemaphoreType.DMA((stages,)),
        ],
        compiler_params=pltpu.CompilerParams(
            collective_id=0, has_side_effects=True, vmem_limit_bytes=60 << 20
        ),
    )(
        left_factor,
        right_factor,
        left_plan,
        right_plan,
        log_inner.reshape(1, columns),
        left_mass.reshape(tiles, LANES),
        right_mass.reshape(tiles, LANES),
    )
    new_left, new_right, new_log_inner = pl.pallas_call(
        finish,
        out_shape=(
            jax.ShapeDtypeStruct((columns, points), F32),
            jax.ShapeDtypeStruct((columns, points), F32),
            jax.ShapeDtypeStruct((1, columns), F32),
        ),
        in_specs=[vmem] * 4,
        out_specs=(hbm, hbm, vmem),
        scratch_shapes=[
            pltpu.VMEM((2 * columns, points), F32),
            pltpu.SemaphoreType.DMA((2,)),
        ],
        compiler_params=pltpu.CompilerParams(vmem_limit_bytes=8 << 20),
    )(
        *(
            pltpu.with_memory_space_constraint(value, pltpu.VMEM)
            for value in (tilted, row_scale, col_scale, new_log_inner)
        )
    )
    return new_left, new_right, new_log_inner.reshape(columns)


def solution(mesh):
    nx = mesh.shape["rank"]
    nc = 2
    ny = 1
    while mesh.shape["rows"] // nc > ny * ny:
        ny *= 2
    nz = mesh.shape["rows"] // (nc * ny)
    split = Mesh(mesh.devices.reshape(ny, nz, nc, nx), ("y", "z", "c", "x"))
    placed = (
        P(None, ROWS),
        P(None, ROWS),
        P("x", ROWS),
        P("x", ROWS),
        P("x"),
        P(ROWS),
        P(ROWS),
    )
    return jax.shard_map(
        functools.partial(per_device, (ny, nz, nc, nx)),
        mesh=split,
        in_specs=placed,
        out_specs=(P("x", ROWS), P("x", ROWS), P("x")),
        check_vma=False,
    )
```
